32 devices in a mesh: ma: 16 (over z, y, core), row: 2 (over x).
Axes of the slice: x: 2, y: 2, z: 4, core: 2. Of those that a mesh axis runs over, the one named last changes fastest.
Arguments:
- spectral: bfloat16 [384, 2, 384, 2, 769], P('ma', None, 'row'), may hold values from -0.011047363 to 0.011047363
- latitude_basis: bfloat16 [384, 769, 1152], P('ma'), may hold values from -0.21875 to 0.21875
- pair_orders: int32 [384], replicated, may hold values from 0 to 383, each once
Outputs:
- grid_values: bfloat16 [64, 2, 1152, 2304], P('row', None, 'ma')
The draws below stay inside these ranges and needn't reach their ends.
Inputs may be any that keep to these rules, and one draw needn't show every extreme that they name: A permutation of 0 to 383; slot p holds the orders pair_orders[p] and 767 - pair_orders[p].
All inputs are finite; a program needn't handle non-finite values.
Results may differ from the reference program's by a relative error of at most 0.0066.
Values may be sent and summed in bfloat16 or wider, within the bound.
No kernel may reach another device: no remote copies, remote signals or barrier semaphores. Data moves between devices by JAX's collectives and lax.ppermute only.
A program may use at most 192 MiB of HBM per device.

```python
import math
import jax
import jax.numpy as jnp
from jax import lax

L = 768
NCHEB = 384
NLAT = 1152
NLON = 2304
FIELDS = 2
LEV = 64
PAIRS = 384
PACKED = 769


def shard_levels(stream_key, dims, shards, smallest, largest):
    def one(axis_at, blocks):
        heights = jax.random.uniform(jax.random.fold_in(jax.random.fold_in(stream_key, 6), axis_at), (blocks,), jnp.float32, smallest / len(shards), largest / len(shards))
        return jnp.repeat(jnp.exp(heights), dims[axis_at] // blocks).reshape((-1,) + (1,) * (len(dims) - axis_at - 1))

    gain = one(*shards[0])
    for cut in shards[1:]:
        gain = gain * one(*cut)
    return gain


def normal_values(rng, extent, width, reach, cuts=(), held_as=jnp.bfloat16):
    factor_of = shard_levels(rng, extent, cuts, -0.22, 0.18) if cuts else 1.0
    array = jax.random.normal(rng, extent, jnp.float32) * width * factor_of
    return jnp.minimum(jnp.maximum(array, -reach), reach).astype(held_as)


def setup_inputs(seed: int = 0) -> dict:
    key_list = jax.random.split(jax.random.key(seed), 4)
    spectral = normal_values(key_list[0], (PAIRS, 2, NCHEB, FIELDS, PACKED), (1.0 / (NCHEB * L) ** 0.5), 0.011047363, ((0, 16), (2, 2)))
    latitude_basis = normal_values(key_list[1], (PAIRS, PACKED, NLAT), PACKED ** -0.5, 0.21875, ((0, 16),))
    pair_orders = jax.random.permutation(key_list[2], PAIRS).astype(jnp.int32)
    return dict(spectral=spectral, latitude_basis=latitude_basis, pair_orders=pair_orders)


def radial_table(total_modes, levels):
    mode_index = lax.broadcasted_iota(jnp.int32, (total_modes, levels), 0)
    points = lax.broadcasted_iota(jnp.int32, (total_modes, levels), 1)
    period = 2 * (total_modes - 1)
    phase_steps = (mode_index * points) % period
    return jnp.cos(phase_steps.astype(jnp.float32) * (2.0 * math.pi / period)).astype(jnp.bfloat16)


def longitude_table(pair_orders, degrees, points):
    lower_orders = pair_orders.astype(jnp.int32)
    orders = jnp.stack([lower_orders, degrees - 1 - lower_orders], axis=1)
    weights = jnp.where(orders == 0, 1.0, 2.0).astype(jnp.float32)
    phase_index = (orders[:, :, None] * lax.broadcasted_iota(jnp.int32, (1, 1, points), 2)) % points
    angles = phase_index.astype(jnp.float32) * (2.0 * math.pi / points)
    real_part = weights[:, :, None] * jnp.cos(angles)
    imag_part = -weights[:, :, None] * jnp.sin(angles)
    stacked = jnp.stack([real_part, imag_part], axis=2)
    return stacked.reshape(-1, points).astype(jnp.bfloat16)


def reference(spectral, latitude_basis, pair_orders):
    cheb_table = radial_table(NCHEB, LEV).astype(jnp.float32)
    lon_table = longitude_table(pair_orders, L, NLON).astype(jnp.float32)
    packed_rows = jnp.arange(PACKED, dtype=jnp.int32)

    def one_pair(pair_index):
        coeffs = lax.dynamic_index_in_dim(spectral, pair_index, 0, keepdims=False)
        basis_rows = lax.dynamic_index_in_dim(latitude_basis, pair_index, 0, keepdims=False)
        lower_order = lax.dynamic_index_in_dim(pair_orders, pair_index, 0, keepdims=False).astype(jnp.int32)
        below_split = packed_rows < (L - lower_order)
        selectors = jnp.stack([below_split, jnp.logical_not(below_split)], axis=0).astype(jnp.float32)
        summed = jnp.einsum("ckfr,kl->lfcr", coeffs.astype(jnp.float32), cheb_table)
        levels = lax.optimization_barrier(summed.astype(jnp.bfloat16)).astype(jnp.float32)
        masked = levels[None] * selectors[:, None, None, None, :]
        fourier = jnp.einsum("hlfcr,rt->lfhct", masked, basis_rows.astype(jnp.float32))
        return fourier.astype(jnp.bfloat16)

    fourier_all = lax.map(one_pair, jnp.arange(PAIRS, dtype=jnp.int32))
    stacked = jnp.transpose(fourier_all, (1, 2, 5, 0, 3, 4)).reshape(LEV, FIELDS, NLAT, PAIRS * 4)

    def one_level(level_block):
        return jnp.einsum("fto,on->ftn", level_block.astype(jnp.float32), lon_table).astype(jnp.bfloat16)

    return lax.map(one_level, stacked)
```

```python
import math

import jax
import jax.numpy as jnp
from jax import lax
from jax.experimental import pallas as pl
from jax.experimental.pallas import tpu as pltpu
from jax.sharding import PartitionSpec as P


NLON = 2304
LEV = 64


def radial_table(total_modes, levels):
    mode_index = lax.broadcasted_iota(jnp.int32, (total_modes, levels), 0)
    points = lax.broadcasted_iota(jnp.int32, (total_modes, levels), 1)
    period = 2 * (total_modes - 1)
    phase_steps = mode_index * points % period
    return jnp.cos(phase_steps.astype(jnp.float32) * (2.0 * math.pi / period)).astype(jnp.bfloat16)


def longitude_kernel(ca_ref, sa_ref, cb_ref, sb_ref, o_ref):
    lanes = cb_ref.shape[1]
    cb, sb = cb_ref[...], sb_ref[...]
    for a in range(o_ref.shape[-1] // lanes):
        ca, sa = ca_ref[:, a : a + 1], sa_ref[:, a : a + 1]
        at = slice(a * lanes, (a + 1) * lanes)
        o_ref[0, :, at] = (ca * cb - sa * sb).astype(jnp.bfloat16)
        o_ref[1, :, at] = -(sa * cb + ca * sb).astype(jnp.bfloat16)


def longitude_rows(pair_orders, degrees, points):
    lanes = 128
    orders = jnp.stack([pair_orders, degrees - 1 - pair_orders], axis=1).reshape(-1, 1)
    weights = jnp.where(orders == 0, 1.0, 2.0).astype(jnp.float32)
    column = lax.broadcasted_iota(jnp.int32, (1, lanes), 1)
    unit = 2.0 * math.pi / points
    coarse = ((orders * (column * lanes % points)) % points).astype(jnp.float32) * unit
    fine = ((orders * column) % points).astype(jnp.float32) * unit
    rows = orders.shape[0]
    block = rows // 2
    small = pl.BlockSpec((block, lanes), lambda i: (i, 0))
    return pl.pallas_call(
        longitude_kernel,
        grid=(rows // block,),
        in_specs=[small] * 4,
        out_specs=pl.BlockSpec((2, block, points), lambda i: (0, i, 0)),
        out_shape=jax.ShapeDtypeStruct((2, rows, points), jnp.bfloat16),
        compiler_params=pltpu.CompilerParams(vmem_limit_bytes=48 * 2**20),
        name="longitude",
    )(weights * jnp.cos(coarse), weights * jnp.sin(coarse), jnp.cos(fine), jnp.sin(fine))


def fourier_kernel(order_ref, basis_ref, kept_ref, got_ref, o_ref, w_ref, m_ref, t_ref, *, start):
    pairs, degrees = kept_ref.shape[0], basis_ref.shape[0] - 1
    half = m_ref.shape[1] // 2
    first = pl.program_id(0) * pairs + start

    @pl.when(pl.program_id(1) == 0)
    def _():
        column = lax.broadcasted_iota(jnp.int32, (half, degrees), 1)
        for p in range(pairs):
            own = kept_ref[p].reshape(half, degrees + 1) + got_ref[p].reshape(half, degrees + 1).astype(jnp.float32)
            own = own.astype(jnp.bfloat16).astype(jnp.float32)
            t_ref[p] = own[:, degrees:]
            own = own[:, :degrees]
            below = column < degrees - order_ref[first + p]
            m_ref[p, :half] = jnp.where(below, own, 0.0).astype(jnp.bfloat16)
            m_ref[p, half:] = jnp.where(below, 0.0, own).astype(jnp.bfloat16)

    rows = 32

    def turn(k, carry):
        at = pl.multiple_of(k * rows, rows)
        x = basis_ref[pl.ds(at, rows)].astype(jnp.float32)
        w_ref[:, pl.ds(at, rows), :] = jnp.transpose(x, (1, 0, 2)).astype(jnp.bfloat16)
        return carry

    lax.fori_loop(0, degrees // rows, turn, 0)
    last = basis_ref[degrees].astype(jnp.float32)
    for p in range(pairs):
        sums = jnp.dot(m_ref[p], w_ref[p], preferred_element_type=jnp.float32)
        tail = t_ref[p] * last[p : p + 1]
        o_ref[p, 0] = sums[:half].astype(jnp.bfloat16).reshape(o_ref.shape[2:])
        o_ref[p, 1] = (sums[half:] + tail).astype(jnp.bfloat16).reshape(o_ref.shape[2:])


def fourier_rows(kept, got, basis, orders, start, level_block):
    pairs, parts, fields, levels, packed = got.shape
    degrees, lat = packed - 1, basis.shape[2]
    width, eight = lat // 3, 8
    block = (eight, parts, fields, levels, packed)
    return pl.pallas_call(
        lambda *refs: fourier_kernel(*refs, start=start),
        grid_spec=pltpu.PrefetchScalarGridSpec(
            num_scalar_prefetch=1,
            grid=(pairs // eight, lat // width),
            in_specs=[
                pl.BlockSpec((packed, eight, width), lambda g, t, _: (0, g + start // eight, t)),
                pl.BlockSpec(block, lambda g, t, _: (g + start // eight, 0, 0, level_block, 0)),
                pl.BlockSpec(block, lambda g, t, _: (g, 0, 0, 0, 0)),
            ],
            out_specs=pl.BlockSpec((eight, 2, parts, fields, levels, width), lambda g, t, _: (g, 0, 0, 0, 0, t)),
            scratch_shapes=[
                pltpu.VMEM((eight, degrees, width), jnp.bfloat16),
                pltpu.VMEM((eight, 2 * parts * fields * levels, degrees), jnp.bfloat16),
                pltpu.VMEM((eight, parts * fields * levels, 1), jnp.float32),
            ],
        ),
        out_shape=jax.ShapeDtypeStruct((pairs, 2, parts, fields, levels, lat), jnp.bfloat16),
        compiler_params=pltpu.CompilerParams(vmem_limit_bytes=56 * 2**20),
        name="fourier",
    )(orders, basis, kept, got)


def pack_kernel(x_ref, *refs, dests, lats, fields):
    outs, s_ref = refs[:-1], refs[-1]
    rows, parts, series, _ = x_ref.shape
    levels = series // fields

    def turn(at, carry):
        c, k = at // (rows // 8), pl.multiple_of(at % (rows // 8) * 8, 8)
        block = jnp.transpose(x_ref[pl.ds(k, 8), c].astype(jnp.float32), (1, 0, 2))
        for i in range(series):
            s_ref[i, c, pl.ds(k, 8), :] = block[i % fields * levels + i // fields]
        return carry

    lax.fori_loop(0, parts * (rows // 8), turn, 0)
    each = outs[0].shape[1]
    group = series // (each * len(outs))
    for n, o_ref in enumerate(outs):

        def spread(at, carry):
            g, c = at // parts, at % parts
            for i in range(group):
                whole = s_ref[(n * each + g) * group + i, c].astype(jnp.bfloat16)
                for d in range(dests):
                    o_ref[d, g, c, :, i * lats : (i + 1) * lats] = whole[:, d * lats : (d + 1) * lats]
            return carry

        lax.fori_loop(0, each * parts, spread, 0)


def pack(fourier, dests, fields, groups, arrays):
    rows, parts, series, lat = fourier.shape
    lats = lat // dests
    block = 16
    shape = (dests, groups // arrays, parts, rows, series // groups * lats)
    return pl.pallas_call(
        lambda x, *refs: pack_kernel(x, *refs, dests=dests, lats=lats, fields=fields),
        grid=(rows // block,),
        in_specs=[pl.BlockSpec((block, parts, series, lat), lambda k: (k, 0, 0, 0))],
        out_specs=[pl.BlockSpec(shape[:3] + (block, shape[4]), lambda k: (0, 0, 0, k, 0))] * arrays,
        out_shape=[jax.ShapeDtypeStruct(shape, jnp.bfloat16)] * arrays,
        scratch_shapes=[pltpu.VMEM((series, parts, block, lat), jnp.float32)],
        compiler_params=pltpu.CompilerParams(vmem_limit_bytes=56 * 2**20),
        name="pack",
    )(fourier)


def synth_kernel(*refs, parts):
    table_ref, out_ref, lhs_ref = refs[parts], *refs[-2:]

    @pl.when(pl.program_id(0) == 0)
    def _():
        at = 0
        for c in range(2):
            for ref in refs[:parts]:
                rows = ref.shape[3]
                few = 128 // rows
                for s in range(0, ref.shape[0], few):
                    x = ref[s : s + few, 0, c].reshape(128, -1)
                    lhs_ref[:, at : at + 128] = jnp.transpose(x)
                    at += 128

    size = lhs_ref.shape[0] // 3

    def some(m, carry):
        at = pl.multiple_of(m * size, size)
        out_ref[pl.ds(at, size), :] = jnp.dot(
            lhs_ref[pl.ds(at, size), :], table_ref[...], preferred_element_type=jnp.float32
        ).astype(jnp.bfloat16)
        return carry

    lax.fori_loop(0, 3, some, 0)


def synthesize(data, table, out, group, groups):
    lanes = data[0][0].shape[-1]
    rows, points = table.shape
    width = 256
    in_specs, operands = [], []
    for x, at in data:
        in_specs.append(pl.BlockSpec((x.shape[0], 1) + x.shape[2:], lambda n, at=at: (0, at, 0, 0, 0)))
        operands.append(x)
    in_specs.append(pl.BlockSpec((rows, width), lambda n: (0, n)))
    operands.append(table)
    parts = len(data)
    aliases = {}
    if out is not None:
        aliases = {len(operands): 0}
        in_specs.append(pl.BlockSpec(memory_space=pl.ANY))
        operands.append(out)
    return pl.pallas_call(
        lambda *refs: synth_kernel(*refs, parts=parts),
        grid=(points // width,),
        in_specs=in_specs,
        out_specs=pl.BlockSpec((lanes, width), lambda n: (group, n)),
        out_shape=jax.ShapeDtypeStruct((groups * lanes, points), jnp.bfloat16),
        scratch_shapes=[pltpu.VMEM((lanes, rows), jnp.bfloat16)],
        input_output_aliases=aliases,
        compiler_params=pltpu.CompilerParams(vmem_limit_bytes=56 * 2**20),
        name="synth",
    )(*operands)


def chunked(spectral, latitude_basis):
    pairs, lats = spectral.shape[0], latitude_basis.shape[2] // lax.axis_size("ma")
    return lax.axis_size("row") == 2 and lats % 8 == 0 and pairs % 8 == 0 and pairs > 8


def per_device(spectral, latitude_basis, pair_orders):
    if chunked(spectral, latitude_basis):
        return per_device_chunked(spectral, latitude_basis, pair_orders)
    return per_device_plain(spectral, latitude_basis, pair_orders)


def per_device_chunked(spectral, latitude_basis, pair_orders):
    pair_dev, _, local_modes, fields, packed = spectral.shape
    degrees = packed - 1
    lat = latitude_basis.shape[2]
    row_count = lax.axis_size("row")
    ma_count = lax.axis_size("ma")
    level_dev = LEV // row_count
    row = lax.axis_index("row")
    mine = lax.axis_index("ma")
    table = radial_table(local_modes * row_count, LEV)
    own_rows = lax.dynamic_slice_in_dim(table, row * local_modes, local_modes, 0)
    own_levels = lax.dynamic_slice_in_dim(own_rows, row * level_dev, level_dev, 1)
    peer_levels = lax.dynamic_slice_in_dim(own_rows, (1 - row) * level_dev, level_dev, 1)
    local_orders = lax.dynamic_slice_in_dim(pair_orders, mine * pair_dev, pair_dev, 0)
    swap = [(0, 1), (1, 0)]

    def radial(columns):
        return jnp.einsum("pckfr,kl->pcflr", spectral, columns, preferred_element_type=jnp.float32)

    sent = radial(peer_levels).astype(jnp.bfloat16)
    kept = radial(own_levels)
    basis = jnp.transpose(latitude_basis, (1, 0, 2))
    groups = 4
    half, eight = level_dev // 2, 8
    chunks = [((0, eight), 0, 1), ((0, eight), 1, 1), ((eight, pair_dev), 0, 1), ((eight, pair_dev), 1, 2)]

    def exchange(x):
        return lax.all_to_all(x, "ma", split_axis=0, concat_axis=0, tiled=True)

    got = []
    for p, l, arrays in chunks:
        peer = lax.ppermute(sent[p[0] : p[1], :, :, l * half : (l + 1) * half], "row", swap)
        sums = fourier_rows(kept, peer, basis, local_orders, p[0], l)
        sums = sums.reshape((p[1] - p[0]) * 2, 2, fields * half, lat)
        packed_rows = pack(sums, ma_count, fields, groups // 2, arrays)
        got += [exchange(x) for x in packed_rows]
    by_owner = pair_orders.reshape(ma_count, pair_dev)
    order_rows = jnp.concatenate([by_owner[:, :eight].reshape(-1), by_owner[:, eight:].reshape(-1)])
    table = longitude_rows(order_rows, degrees, NLON).reshape(-1, NLON)
    out = None
    for g in range(groups):
        data = [(got[g // 2], g % 2), (got[2], g) if g < 2 else (got[1 + g], 0)]
        out = synthesize(data, table, out, g, groups)
    return out.reshape(level_dev, fields, lat // ma_count, NLON)


def longitude_table(pair_orders, degrees, points):
    orders = jnp.stack([pair_orders, degrees - 1 - pair_orders], axis=1)
    weights = jnp.where(orders == 0, 1.0, 2.0).astype(jnp.float32)
    phase_index = orders[:, :, None] * lax.broadcasted_iota(jnp.int32, (1, 1, points), 2) % points
    angles = phase_index.astype(jnp.float32) * (2.0 * math.pi / points)
    real_part = weights[:, :, None] * jnp.cos(angles)
    imag_part = -weights[:, :, None] * jnp.sin(angles)
    stacked = jnp.stack([real_part, imag_part], axis=2)
    return stacked.reshape(-1, points).astype(jnp.bfloat16)


def order_selectors(local_orders, degrees, packed):
    packed_rows = lax.broadcasted_iota(jnp.int32, (local_orders.shape[0], packed), 1)
    below_split = packed_rows < (degrees - local_orders)[:, None]
    return jnp.stack([below_split, jnp.logical_not(below_split)], axis=1).astype(jnp.bfloat16)


def per_device_plain(spectral, latitude_basis, pair_orders):
    pair_dev = spectral.shape[0]
    local_modes = spectral.shape[2]
    fields = spectral.shape[3]
    packed = spectral.shape[4]
    degrees = packed - 1
    row_count = lax.axis_size("row")
    total_modes = local_modes * row_count
    level_dev = LEV // row_count
    cheb_table = radial_table(total_modes, LEV)
    own_rows = lax.dynamic_slice_in_dim(
        cheb_table, lax.axis_index("row") * local_modes, local_modes, 0
    )
    scattered = lax.psum_scatter(
        jnp.einsum("pckfr,kl->lpcfr", spectral, own_rows, preferred_element_type=jnp.float32),
        "row",
        scatter_dimension=0,
        tiled=True,
    )
    summed = jnp.transpose(scattered, (1, 2, 0, 3, 4))
    levels = summed.astype(jnp.bfloat16)
    local_orders = lax.dynamic_slice_in_dim(
        pair_orders, lax.axis_index("ma") * pair_dev, pair_dev, 0
    )
    selectors = order_selectors(local_orders, degrees, packed)
    masked = levels[:, None] * selectors[:, :, None, None, None, :]
    lon_table = longitude_table(pair_orders, degrees, NLON)
    block_levels = masked.shape[3]
    fourier = jnp.einsum(
        "phclfr,prt->phclft", masked, latitude_basis, preferred_element_type=jnp.float32
    ).astype(jnp.bfloat16)
    fourier = fourier.reshape(pair_dev * 4, block_levels * fields, fourier.shape[-1])
    synthesized = jnp.einsum(
        "oit,on->itn",
        lax.all_to_all(fourier, "ma", split_axis=2, concat_axis=0, tiled=True),
        lon_table,
        preferred_element_type=jnp.float32,
    ).astype(jnp.bfloat16)
    return synthesized.reshape(level_dev, fields, synthesized.shape[1], synthesized.shape[2])


def solution(mesh):
    return jax.shard_map(
        per_device,
        mesh=mesh,
        in_specs=(P("ma", None, "row", None, None), P("ma", None, None), P()),
        out_specs=P("row", None, "ma", None),
        check_vma=False,
    )
```

```python
import math

import jax
import jax.numpy as jnp
from jax import lax
from jax.experimental import pallas as pl
from jax.experimental.pallas import tpu as pltpu
from jax.sharding import PartitionSpec as P


NLON = 2304
LEV = 64


def radial_table(total_modes, levels):
    mode_index = lax.broadcasted_iota(jnp.int32, (total_modes, levels), 0)
    points = lax.broadcasted_iota(jnp.int32, (total_modes, levels), 1)
    period = 2 * (total_modes - 1)
    phase_steps = mode_index * points % period
    return jnp.cos(phase_steps.astype(jnp.float32) * (2.0 * math.pi / period)).astype(jnp.bfloat16)


def longitude_kernel(ca_ref, sa_ref, cb_ref, sb_ref, o_ref):
    lanes = cb_ref.shape[1]
    cb, sb = cb_ref[...], sb_ref[...]
    for a in range(o_ref.shape[-1] // lanes):
        ca, sa = ca_ref[:, a : a + 1], sa_ref[:, a : a + 1]
        at = slice(a * lanes, (a + 1) * lanes)
        o_ref[0, :, at] = (ca * cb - sa * sb).astype(jnp.bfloat16)
        o_ref[1, :, at] = -(sa * cb + ca * sb).astype(jnp.bfloat16)


def longitude_rows(pair_orders, degrees, points):
    lanes = 128
    orders = jnp.stack([pair_orders, degrees - 1 - pair_orders], axis=1).reshape(-1, 1)
    weights = jnp.where(orders == 0, 1.0, 2.0).astype(jnp.float32)
    column = lax.broadcasted_iota(jnp.int32, (1, lanes), 1)
    unit = 2.0 * math.pi / points
    coarse = ((orders * (column * lanes % points)) % points).astype(jnp.float32) * unit
    fine = ((orders * column) % points).astype(jnp.float32) * unit
    rows = orders.shape[0]
    block = rows // 2
    small = pl.BlockSpec((block, lanes), lambda i: (i, 0))
    return pl.pallas_call(
        longitude_kernel,
        grid=(rows // block,),
        in_specs=[small] * 4,
        out_specs=pl.BlockSpec((2, block, points), lambda i: (0, i, 0)),
        out_shape=jax.ShapeDtypeStruct((2, rows, points), jnp.bfloat16),
        compiler_params=pltpu.CompilerParams(vmem_limit_bytes=48 * 2**20),
        name="longitude",
    )(weights * jnp.cos(coarse), weights * jnp.sin(coarse), jnp.cos(fine), jnp.sin(fine))


def fourier_kernel(order_ref, basis_ref, kept_ref, got_ref, o_ref, w_ref, m_ref, t_ref, *, start):
    pairs, degrees = kept_ref.shape[0], basis_ref.shape[0] - 1
    half = m_ref.shape[1] // 2
    first = pl.program_id(0) * pairs + start

    @pl.when(pl.program_id(1) == 0)
    def _():
        column = lax.broadcasted_iota(jnp.int32, (half, degrees), 1)
        for p in range(pairs):
            own = kept_ref[p].reshape(half, degrees + 1) + got_ref[p].reshape(half, degrees + 1).astype(jnp.float32)
            own = own.astype(jnp.bfloat16).astype(jnp.float32)
            t_ref[p] = own[:, degrees:]
            own = own[:, :degrees]
            below = column < degrees - order_ref[first + p]
            m_ref[p, :half] = jnp.where(below, own, 0.0).astype(jnp.bfloat16)
            m_ref[p, half:] = jnp.where(below, 0.0, own).astype(jnp.bfloat16)

    rows = 32

    def turn(k, carry):
        at = pl.multiple_of(k * rows, rows)
        x = basis_ref[pl.ds(at, rows)].astype(jnp.float32)
        w_ref[:, pl.ds(at, rows), :] = jnp.transpose(x, (1, 0, 2)).astype(jnp.bfloat16)
        return carry

    lax.fori_loop(0, degrees // rows, turn, 0)
    last = basis_ref[degrees].astype(jnp.float32)
    for p in range(pairs):
        sums = jnp.dot(m_ref[p], w_ref[p], preferred_element_type=jnp.float32)
        tail = t_ref[p] * last[p : p + 1]
        o_ref[p, 0] = sums[:half].astype(jnp.bfloat16).reshape(o_ref.shape[2:])
        o_ref[p, 1] = (sums[half:] + tail).astype(jnp.bfloat16).reshape(o_ref.shape[2:])


def fourier_rows(kept, got, basis, orders, start, level_block):
    pairs, parts, fields, levels, packed = got.shape
    degrees, lat = packed - 1, basis.shape[2]
    width, eight = lat // 3, 8
    block = (eight, parts, fields, levels, packed)
    return pl.pallas_call(
        lambda *refs: fourier_kernel(*refs, start=start),
        grid_spec=pltpu.PrefetchScalarGridSpec(
            num_scalar_prefetch=1,
            grid=(pairs // eight, lat // width),
            in_specs=[
                pl.BlockSpec((packed, eight, width), lambda g, t, _: (0, g + start // eight, t)),
                pl.BlockSpec(block, lambda g, t, _: (g + start // eight, 0, 0, level_block, 0)),
                pl.BlockSpec(block, lambda g, t, _: (g, 0, 0, 0, 0)),
            ],
            out_specs=pl.BlockSpec((eight, 2, parts, fields, levels, width), lambda g, t, _: (g, 0, 0, 0, 0, t)),
            scratch_shapes=[
                pltpu.VMEM((eight, degrees, width), jnp.bfloat16),
                pltpu.VMEM((eight, 2 * parts * fields * levels, degrees), jnp.bfloat16),
                pltpu.VMEM((eight, parts * fields * levels, 1), jnp.float32),
            ],
        ),
        out_shape=jax.ShapeDtypeStruct((pairs, 2, parts, fields, levels, lat), jnp.bfloat16),
        compiler_params=pltpu.CompilerParams(vmem_limit_bytes=56 * 2**20),
        name="fourier",
    )(orders, basis, kept, got)


def pack_kernel(x_ref, *refs, dests, lats, fields):
    outs, s_ref = refs[:-1], refs[-1]
    rows, parts, series, _ = x_ref.shape
    levels = series // fields

    def turn(at, carry):
        c, k = at // (rows // 8), pl.multiple_of(at % (rows // 8) * 8, 8)
        block = jnp.transpose(x_ref[pl.ds(k, 8), c].astype(jnp.float32), (1, 0, 2))
        for i in range(series):
            s_ref[i, c, pl.ds(k, 8), :] = block[i % fields * levels + i // fields]
        return carry

    lax.fori_loop(0, parts * (rows // 8), turn, 0)
    each = outs[0].shape[1]
    group = series // (each * len(outs))
    for n, o_ref in enumerate(outs):

        def spread(at, carry):
            g, c = at // parts, at % parts
            for i in range(group):
                whole = s_ref[(n * each + g) * group + i, c].astype(jnp.bfloat16)
                for d in range(dests):
                    o_ref[d, g, c, :, i * lats : (i + 1) * lats] = whole[:, d * lats : (d + 1) * lats]
            return carry

        lax.fori_loop(0, each * parts, spread, 0)


def pack(fourier, dests, fields, groups, arrays):
    rows, parts, series, lat = fourier.shape
    lats = lat // dests
    block = 16
    shape = (dests, groups // arrays, parts, rows, series // groups * lats)
    return pl.pallas_call(
        lambda x, *refs: pack_kernel(x, *refs, dests=dests, lats=lats, fields=fields),
        grid=(rows // block,),
        in_specs=[pl.BlockSpec((block, parts, series, lat), lambda k: (k, 0, 0, 0))],
        out_specs=[pl.BlockSpec(shape[:3] + (block, shape[4]), lambda k: (0, 0, 0, k, 0))] * arrays,
        out_shape=[jax.ShapeDtypeStruct(shape, jnp.bfloat16)] * arrays,
        scratch_shapes=[pltpu.VMEM((series, parts, block, lat), jnp.float32)],
        compiler_params=pltpu.CompilerParams(vmem_limit_bytes=56 * 2**20),
        name="pack",
    )(fourier)


def synth_kernel(*refs, parts):
    table_ref, out_ref, lhs_ref = refs[parts], *refs[-2:]

    @pl.when(pl.program_id(1) == 0)
    def _():
        at = 0
        for c in range(2):
            for ref in refs[:parts]:
                rows = ref.shape[3]
                few = 128 // rows
                for s in range(0, ref.shape[0], few):
                    x = ref[s : s + few, 0, c].reshape(128, -1)
                    lhs_ref[:, at : at + 128] = jnp.transpose(x)
                    at += 128

    size = lhs_ref.shape[0] // 3

    def some(m, carry):
        at = pl.multiple_of(m * size, size)
        out_ref[pl.ds(at, size), :] = jnp.dot(
            lhs_ref[pl.ds(at, size), :], table_ref[...], preferred_element_type=jnp.float32
        ).astype(jnp.bfloat16)
        return carry

    lax.fori_loop(0, 3, some, 0)


def synthesize(data, table, out, group, count, groups):
    lanes = data[0][0].shape[-1]
    rows, points = table.shape
    width = 256
    in_specs, operands = [], []
    for x, at in data:
        in_specs.append(pl.BlockSpec((x.shape[0], 1) + x.shape[2:], lambda g, n, at=at: (0, at + g, 0, 0, 0)))
        operands.append(x)
    in_specs.append(pl.BlockSpec((rows, width), lambda g, n: (0, n)))
    operands.append(table)
    parts = len(data)
    aliases = {}
    if out is not None:
        aliases = {len(operands): 0}
        in_specs.append(pl.BlockSpec(memory_space=pl.ANY))
        operands.append(out)
    return pl.pallas_call(
        lambda *refs: synth_kernel(*refs, parts=parts),
        grid=(count, points // width),
        in_specs=in_specs,
        out_specs=pl.BlockSpec((lanes, width), lambda g, n: (group + g, n)),
        out_shape=jax.ShapeDtypeStruct((groups * lanes, points), jnp.bfloat16),
        scratch_shapes=[pltpu.VMEM((lanes, rows), jnp.bfloat16)],
        input_output_aliases=aliases,
        compiler_params=pltpu.CompilerParams(vmem_limit_bytes=56 * 2**20),
        name="synth",
    )(*operands)


def chunked(spectral, latitude_basis):
    pairs, lats = spectral.shape[0], latitude_basis.shape[2] // lax.axis_size("ma")
    return lax.axis_size("row") == 2 and lats % 8 == 0 and pairs % 8 == 0 and pairs > 8


def per_device(spectral, latitude_basis, pair_orders):
    if chunked(spectral, latitude_basis):
        return per_device_chunked(spectral, latitude_basis, pair_orders)
    return per_device_plain(spectral, latitude_basis, pair_orders)


def per_device_chunked(spectral, latitude_basis, pair_orders):
    pair_dev, _, local_modes, fields, packed = spectral.shape
    degrees = packed - 1
    lat = latitude_basis.shape[2]
    row_count = lax.axis_size("row")
    ma_count = lax.axis_size("ma")
    level_dev = LEV // row_count
    row = lax.axis_index("row")
    mine = lax.axis_index("ma")
    table = radial_table(local_modes * row_count, LEV)
    own_rows = lax.dynamic_slice_in_dim(table, row * local_modes, local_modes, 0)
    own_levels = lax.dynamic_slice_in_dim(own_rows, row * level_dev, level_dev, 1)
    peer_levels = lax.dynamic_slice_in_dim(own_rows, (1 - row) * level_dev, level_dev, 1)
    local_orders = lax.dynamic_slice_in_dim(pair_orders, mine * pair_dev, pair_dev, 0)
    swap = [(0, 1), (1, 0)]

    def radial(coeffs, columns):
        return jnp.einsum("pckfr,kl->pcflr", coeffs, columns, preferred_element_type=jnp.float32)

    early = lax.optimization_barrier(spectral[:8])
    sent0 = radial(early, peer_levels).astype(jnp.bfloat16)
    kept0 = radial(early, own_levels)
    both = radial(spectral, jnp.concatenate([peer_levels, own_levels], axis=1))
    basis = jnp.transpose(latitude_basis, (1, 0, 2))
    groups = 4
    half, eight = level_dev // 2, 8
    chunks = [((0, eight), 0, 1), ((0, eight), 1, 1), ((eight, pair_dev), 0, 1), ((eight, pair_dev), 1, 2)]

    def exchange(x):
        return lax.all_to_all(x, "ma", split_axis=0, concat_axis=0, tiled=True)

    got = []
    for p, l, arrays in chunks:
        sent, kept, kept_at = (both, both, l + 2) if p[0] else (sent0, kept0, l)
        sent = sent[p[0] : p[1], :, :, l * half : (l + 1) * half].astype(jnp.bfloat16)
        peer = lax.ppermute(sent, "row", swap)
        sums = fourier_rows(kept, peer, basis, local_orders, p[0], kept_at)
        sums = sums.reshape((p[1] - p[0]) * 2, 2, fields * half, lat)
        packed_rows = pack(sums, ma_count, fields, groups // 2, arrays)
        got += [exchange(x) for x in packed_rows]
    by_owner = pair_orders.reshape(ma_count, pair_dev)
    order_rows = jnp.concatenate([by_owner[:, :eight].reshape(-1), by_owner[:, eight:].reshape(-1)])
    table = longitude_rows(order_rows, degrees, NLON).reshape(-1, NLON)
    out = None
    for at, (g, count) in enumerate(((0, 2), (2, 1), (3, 1))):
        data = [(got[g // 2], g % 2), (got[2 + at], 0)]
        out = synthesize(data, table, out, g, count, groups)
    return out.reshape(level_dev, fields, lat // ma_count, NLON)


def longitude_table(pair_orders, degrees, points):
    orders = jnp.stack([pair_orders, degrees - 1 - pair_orders], axis=1)
    weights = jnp.where(orders == 0, 1.0, 2.0).astype(jnp.float32)
    phase_index = orders[:, :, None] * lax.broadcasted_iota(jnp.int32, (1, 1, points), 2) % points
    angles = phase_index.astype(jnp.float32) * (2.0 * math.pi / points)
    real_part = weights[:, :, None] * jnp.cos(angles)
    imag_part = -weights[:, :, None] * jnp.sin(angles)
    stacked = jnp.stack([real_part, imag_part], axis=2)
    return stacked.reshape(-1, points).astype(jnp.bfloat16)


def order_selectors(local_orders, degrees, packed):
    packed_rows = lax.broadcasted_iota(jnp.int32, (local_orders.shape[0], packed), 1)
    below_split = packed_rows < (degrees - local_orders)[:, None]
    return jnp.stack([below_split, jnp.logical_not(below_split)], axis=1).astype(jnp.bfloat16)


def per_device_plain(spectral, latitude_basis, pair_orders):
    pair_dev = spectral.shape[0]
    local_modes = spectral.shape[2]
    fields = spectral.shape[3]
    packed = spectral.shape[4]
    degrees = packed - 1
    row_count = lax.axis_size("row")
    total_modes = local_modes * row_count
    level_dev = LEV // row_count
    cheb_table = radial_table(total_modes, LEV)
    own_rows = lax.dynamic_slice_in_dim(
        cheb_table, lax.axis_index("row") * local_modes, local_modes, 0
    )
    scattered = lax.psum_scatter(
        jnp.einsum("pckfr,kl->lpcfr", spectral, own_rows, preferred_element_type=jnp.float32),
        "row",
        scatter_dimension=0,
        tiled=True,
    )
    summed = jnp.transpose(scattered, (1, 2, 0, 3, 4))
    levels = summed.astype(jnp.bfloat16)
    local_orders = lax.dynamic_slice_in_dim(
        pair_orders, lax.axis_index("ma") * pair_dev, pair_dev, 0
    )
    selectors = order_selectors(local_orders, degrees, packed)
    masked = levels[:, None] * selectors[:, :, None, None, None, :]
    lon_table = longitude_table(pair_orders, degrees, NLON)
    block_levels = masked.shape[3]
    fourier = jnp.einsum(
        "phclfr,prt->phclft", masked, latitude_basis, preferred_element_type=jnp.float32
    ).astype(jnp.bfloat16)
    fourier = fourier.reshape(pair_dev * 4, block_levels * fields, fourier.shape[-1])
    synthesized = jnp.einsum(
        "oit,on->itn",
        lax.all_to_all(fourier, "ma", split_axis=2, concat_axis=0, tiled=True),
        lon_table,
        preferred_element_type=jnp.float32,
    ).astype(jnp.bfloat16)
    return synthesized.reshape(level_dev, fields, synthesized.shape[1], synthesized.shape[2])


def solution(mesh):
    return jax.shard_map(
        per_device,
        mesh=mesh,
        in_specs=(P("ma", None, "row", None, None), P("ma", None, None), P()),
        out_specs=P("row", None, "ma", None),
        check_vma=False,
    )
```
